32 devices in a mesh: dp: 4 (over x, core), ctx: 2 (over y), tensor: 4 (over z).
Axes of the slice: x: 2, y: 2, z: 4, core: 2. Of those that a mesh axis runs over, the one named last changes fastest.
Arguments:
- layer_input: bfloat16 [8192, 2048], P(('dp', 'ctx')), may hold values from -6 to 6
- attention_gain: float32 [2048], replicated, may hold values from 0.5 to 1.5
- attention_shift: float32 [2048], replicated, may hold values from -4 to 4
- feed_gain: float32 [2048], replicated, may hold values from 0.5 to 1.5
- feed_shift: float32 [2048], replicated, may hold values from -4 to 4
- qkv_weight: bfloat16 [2048, 6144], P('dp', 'tensor'), may hold values from -0.125 to 0.125
- qkv_bias: float32 [6144], P('tensor'), may hold values from -16 to 16
- dense_weight: bfloat16 [2048, 2048], P('tensor', 'dp'), may hold values from -0.5 to 0.5
- up_weight: bfloat16 [2048, 8192], P('dp', 'tensor'), may hold values from -0.125 to 0.125
- up_bias: float32 [8192], P('tensor'), may hold values from -6 to 6
- down_weight: bfloat16 [8192, 2048], P('tensor', 'dp'), may hold values from -0.0625 to 0.0625
- out_bias: float32 [2048], replicated, may hold values from -6 to 6
- segment_ids: int32 [4, 2048], P('dp', 'ctx'), may hold values from 0 to 3, never falling along the last dimension, each value on 1 to 1536 neighbouring positions
- out_cotangent: bfloat16 [8192, 2048], P(('dp', 'ctx')), may hold values from -6 to 6
Outputs:
- layer_output: bfloat16 [8192, 2048], P(('dp', 'ctx'))
- input_grad: float32 [8192, 2048], P(('dp', 'ctx'))
- attention_gain_grad: float32 [2048], replicated
- attention_shift_grad: float32 [2048], replicated
- feed_gain_grad: float32 [2048], replicated
- feed_shift_grad: float32 [2048], replicated
- qkv_weight_grad: float32 [2048, 6144], P('dp', 'tensor')
- qkv_bias_grad: float32 [6144], P('tensor')
- dense_weight_grad: float32 [2048, 2048], P('tensor', 'dp')
- up_weight_grad: float32 [2048, 8192], P('dp', 'tensor')
- up_bias_grad: float32 [8192], P('tensor')
- down_weight_grad: float32 [8192, 2048], P('tensor', 'dp')
- out_bias_grad: float32 [2048], replicated
The draws below stay inside these ranges and needn't reach their ends.
Inputs may be any that keep to these rules, and one draw needn't show every extreme that they name: `segment_ids`: segment ids never fall along a row; each packed row starts with document 0.
All inputs are finite; a program needn't handle non-finite values.
Results may differ from the reference program's by a relative error of at most 0.024.
The reference program's roundings to bfloat16 on the way count: a program that leaves them out, or rounds other values in their place, can miss the bound.
Values may be sent and summed in bfloat16 or wider, within the bound.
A program may use at most 256 MiB of HBM per device.

```python
import math
import jax
import jax.numpy as jnp
import numpy as np
from jax import lax

D = 2048
HEADS = 8
FF = 8192
SEQ_LEN = 2048
HEAD_DIM = 256
ROTARY = 64
SEQS = 4
TOKENS = 8192
N_CTX = 2


def draw_qkv_bias(key, part):
    noise_key = jax.random.fold_in(jax.random.fold_in(key, 7), 0)
    result = jnp.clip(0.5 * jax.random.normal(noise_key, (HEADS, 3, HEAD_DIM), jnp.float32), -3.0, 3.0)
    return result.reshape(3 * D).astype(jnp.float32)


def strengthened(drawn, key, source, target, parts, factor):
    owner, partner = [(jnp.arange(drawn.shape[dim]) // (drawn.shape[dim] // parts)).reshape([-1 if axis == dim else 1 for axis in range(drawn.ndim)]) for dim in (source, target)]
    chosen = jax.random.permutation(key, parts)[partner]
    strong = (owner == chosen) | (owner == (partner + parts // 2) % parts)
    return jnp.where(strong, factor * drawn, drawn)


def level_of(rng, shape, pieces, low, largest):
    level, own = 1.0, jax.random.fold_in(rng, 6)
    for axis_at, shards_of in pieces:
        draws = jnp.exp(jax.random.uniform(jax.random.fold_in(own, axis_at), (shards_of,), jnp.float32, low / len(pieces), largest / len(pieces)))
        level = level * jnp.repeat(draws, shape[axis_at] // shards_of).reshape([-1 if axis == axis_at else 1 for axis in range(len(shape))])
    return level


def split_up(amount, total, most, skew):
    portions = [(1 << 20) // math.isqrt(rank ** skew) + 1 for rank in range(2, amount + 1)]
    rest, holding = total - most - (amount - 1), [1] * (amount - 1)
    while rest > 0:
        candidates = [i for i in range(amount - 1) if holding[i] < most]
        whole, remaining = sum([portions[i] for i in candidates]), rest
        for i in candidates:
            extra = min(most - holding[i], max(1, remaining * portions[i] // whole), rest)
            holding[i] = holding[i] + extra
            rest = rest - extra
    return np.array([most] + holding)


def ragged_sizes(own_key, amount, total, limit, lean):
    if amount == 2:
        one = jax.random.randint(own_key, (), max(1, total - limit), min(limit, total - 1) + 1)
        return jnp.stack([one, total - one])
    sizes = jnp.asarray(split_up(amount, total, limit, lean), jnp.int32)
    twos = (amount - 1) // 2
    giver, receiver = sizes[1:1 + 2 * twos:2], sizes[2:2 + 2 * twos:2]
    slack = jnp.minimum(giver - 1, limit - receiver)
    shifted = jax.random.randint(jax.random.fold_in(own_key, 1), (twos,), 0, 1 << 20) % (slack + 1)
    sizes = sizes.at[1:1 + 2 * twos:2].set(giver - shifted).at[2:2 + 2 * twos:2].set(receiver + shifted)
    return sizes[jax.random.permutation(jax.random.fold_in(own_key, 2), amount)]


def centred(stream_key, dims, width, reach, pieces=(), dtype=jnp.bfloat16):
    factor_of = level_of(stream_key, dims, pieces, -0.22, 0.18) if pieces else 1.0
    drawn = jax.random.normal(stream_key, dims, jnp.float32) * width * factor_of
    return jnp.minimum(jnp.maximum(drawn, -reach), reach).astype(dtype)


def heavy_noise(own_key, dims, deviation, bound, pieces, heavy, kind=jnp.bfloat16):
    array = deviation * jax.random.normal(own_key, dims, jnp.float32)
    if pieces:
        array = array * level_of(own_key, dims, pieces, -0.22, 0.18)
    return jnp.clip(strengthened(array, jax.random.fold_in(own_key, 3), *heavy), -bound, bound).astype(kind)


def setup_inputs(seed: int = 0) -> dict:
    arg_keys = jax.random.split(jax.random.key(seed), 15)
    return {
        "layer_input": centred(arg_keys[0], (TOKENS, D), 1.0, 6.0, ((0, 8),)),
        "attention_gain": jnp.clip(1.0 + 0.1 * jax.random.normal(arg_keys[1], (D,), jnp.float32), 0.5, 1.5),
        "attention_shift": centred(arg_keys[2], (D,), 0.3, 4.0, (), jnp.float32),
        "feed_gain": jnp.clip(1.0 + 0.1 * jax.random.normal(arg_keys[3], (D,), jnp.float32), 0.5, 1.5),
        "feed_shift": centred(arg_keys[4], (D,), 0.3, 4.0, (), jnp.float32),
        "qkv_weight": centred(arg_keys[5], (D, 3 * D), D ** -0.5, 0.125, ((0, 4), (1, 4))),
        "qkv_bias": draw_qkv_bias(jax.random.fold_in(arg_keys[14], 71), 0),
        "dense_weight": centred(arg_keys[7], (D, D), (D // 16) ** -0.5, 0.5, ((0, 4), (1, 4))),
        "up_weight": centred(arg_keys[8], (D, FF), D ** -0.5, 0.125, ((0, 4), (1, 4))),
        "up_bias": centred(arg_keys[9], (FF,), 0.5, 6.0, ((0, 4),), jnp.float32),
        "down_weight": centred(arg_keys[10], (FF, D), FF ** -0.5, 0.0625, ((0, 4), (1, 4))),
        "out_bias": centred(arg_keys[11], (D,), 0.5, 6.0, (), jnp.float32),
        "segment_ids": jax.vmap(lambda own: jnp.searchsorted(jnp.cumsum(ragged_sizes(own, 4, SEQ_LEN, SEQ_LEN // 2 + SEQ_LEN // 4, 2)), jnp.arange(SEQ_LEN), side="right"))(jax.random.split(arg_keys[12], SEQS)).reshape((SEQS, SEQ_LEN)).astype(jnp.int32),
        "out_cotangent": heavy_noise(arg_keys[13], (TOKENS, D), 1.0, 6.0, ((0, 8),), (0, 1, 8, 2.0)),
    }


EPS = 1e-05
SQRT_HALF = 0.7071067811865476
INV_ROOT_TAU = 0.3989422804014327
MASKED = -1e+30

def normalize(rows):
    mean = lax.optimization_barrier(jnp.mean(rows, axis=-1, keepdims=True))
    centered = rows - mean
    variance = lax.optimization_barrier(jnp.mean(centered * centered, axis=-1, keepdims=True))
    scale = lax.rsqrt(variance + EPS)
    return (centered * scale, scale)

def gelu_parts(pre):
    cdf = 0.5 * (1.0 + lax.erf(pre * SQRT_HALF))
    return (pre * cdf, cdf + pre * jnp.exp(-0.5 * pre * pre) * INV_ROOT_TAU)

def rotary_tables(positions, rotary):
    half = rotary // 2
    freq = 10000.0 ** (-2.0 * jnp.arange(half).astype(jnp.float32) / rotary)
    angle = positions.astype(jnp.float32)[:, None] * freq[None, :]
    return (jnp.cos(angle)[:, None, :], jnp.sin(angle)[:, None, :])

def rotate(values, cosine, sine, rotary, sign):
    half = rotary // 2
    first = values[..., :half]
    second = values[..., half:rotary]
    turned = sine * sign
    return jnp.concatenate([first * cosine - second * turned, second * cosine + first * turned, values[..., rotary:]], axis=-1)

def masked_scores(queries, keys, valid, scale):
    scores = jnp.einsum('qhd,khd->hqk', queries.astype(jnp.float32), keys.astype(jnp.float32)) * scale
    return jnp.where(valid[None], scores, MASKED)

def block_term(left, right):
    left_blocks = left.astype(jnp.float32).reshape(N_CTX, -1, left.shape[-1])
    right_blocks = right.astype(jnp.float32).reshape(N_CTX, -1, right.shape[-1])
    terms = jnp.einsum('cti,ctj->cij', left_blocks, right_blocks)
    rounded = lax.optimization_barrier(terms.astype(jnp.bfloat16))
    return lax.optimization_barrier(jnp.sum(rounded.astype(jnp.float32), axis=0))

def reference(layer_input, attention_gain, attention_shift, feed_gain, feed_shift, qkv_weight, qkv_bias, dense_weight, up_weight, up_bias, down_weight, out_bias, segment_ids, out_cotangent):
    scale = HEAD_DIM ** (-0.5)
    positions = jnp.arange(SEQ_LEN).astype(jnp.int32)
    cosine, sine = rotary_tables(positions, ROTARY)
    causal = positions[None, :] <= positions[:, None]

    def one_row(carry, item):
        row_input, row_segments, row_cotangent = item
        inputs = row_input.astype(jnp.float32)
        normed, inv_scale = normalize(inputs)
        attend_in = (normed * attention_gain + attention_shift).astype(jnp.bfloat16)
        feed_in = (normed * feed_gain + feed_shift).astype(jnp.bfloat16)
        projected = (jnp.dot(attend_in, qkv_weight, preferred_element_type=jnp.float32) + qkv_bias).reshape(SEQ_LEN, HEADS, 3, HEAD_DIM)
        queries = rotate(projected[:, :, 0], cosine, sine, ROTARY, 1.0).astype(jnp.bfloat16)
        keys = rotate(projected[:, :, 1], cosine, sine, ROTARY, 1.0).astype(jnp.bfloat16)
        values = projected[:, :, 2].astype(jnp.bfloat16)
        valid = (row_segments[:, None] == row_segments[None, :]) & causal
        scores = masked_scores(queries, keys, valid, scale)
        top = lax.optimization_barrier(jnp.max(scores, axis=-1, keepdims=True))
        lse = top + jnp.log(lax.optimization_barrier(jnp.sum(jnp.exp(scores - top), axis=-1, keepdims=True)))
        probs = jnp.exp(scores - lse).astype(jnp.bfloat16)
        context = jnp.einsum('hqk,khd->qhd', probs.astype(jnp.float32), values.astype(jnp.float32)).astype(jnp.bfloat16).reshape(SEQ_LEN, D)
        pre = jnp.dot(feed_in, up_weight, preferred_element_type=jnp.float32) + up_bias
        activated, slope = gelu_parts(pre)
        activated = activated.astype(jnp.bfloat16)
        attend_out = jnp.dot(context, dense_weight, preferred_element_type=jnp.float32)
        feed_out = jnp.dot(activated, down_weight, preferred_element_type=jnp.float32)
        row_output = (inputs + attend_out + feed_out + out_bias).astype(jnp.bfloat16)
        cotangent = row_cotangent.astype(jnp.float32)
        out_bias_part = lax.optimization_barrier(jnp.sum(cotangent, axis=0))
        hidden_grad = jnp.dot(row_cotangent, down_weight.T, preferred_element_type=jnp.float32) * slope
        up_bias_part = lax.optimization_barrier(jnp.sum(hidden_grad, axis=0))
        hidden_low = hidden_grad.astype(jnp.bfloat16)
        feed_grad = jnp.dot(hidden_low, up_weight.T, preferred_element_type=jnp.float32)
        context_grad = jnp.dot(row_cotangent, dense_weight.T, preferred_element_type=jnp.float32).astype(jnp.bfloat16).reshape(SEQ_LEN, HEADS, HEAD_DIM)
        probs_again = jnp.exp(masked_scores(queries, keys, valid, scale) - lse)
        value_grad = jnp.einsum('hqk,qhd->khd', probs_again.astype(jnp.bfloat16).astype(jnp.float32), context_grad.astype(jnp.float32))
        prob_grad = jnp.einsum('qhd,khd->hqk', context_grad.astype(jnp.float32), values.astype(jnp.float32))
        delta = lax.optimization_barrier(jnp.sum(context_grad.astype(jnp.float32) * context.reshape(SEQ_LEN, HEADS, HEAD_DIM).astype(jnp.float32), axis=-1))
        score_grad = (probs_again * (prob_grad - jnp.transpose(delta)[:, :, None])).astype(jnp.bfloat16).astype(jnp.float32)
        query_grad = jnp.einsum('hqk,khd->qhd', score_grad, keys.astype(jnp.float32)) * scale
        key_grad = jnp.einsum('hqk,qhd->khd', score_grad, queries.astype(jnp.float32)) * scale
        query_grad = rotate(query_grad, cosine, sine, ROTARY, -1.0)
        key_grad = rotate(key_grad, cosine, sine, ROTARY, -1.0)
        projected_grad = jnp.stack([query_grad, key_grad, value_grad], axis=2).reshape(SEQ_LEN, 3 * D)
        qkv_bias_part = lax.optimization_barrier(jnp.sum(projected_grad, axis=0))
        projected_low = projected_grad.astype(jnp.bfloat16)
        attend_grad = jnp.dot(projected_low, qkv_weight.T, preferred_element_type=jnp.float32)
        normed_grad = attend_grad * attention_gain + feed_grad * feed_gain
        row_input_grad = cotangent + inv_scale * (normed_grad - lax.optimization_barrier(jnp.mean(normed_grad, axis=-1, keepdims=True)) - normed * lax.optimization_barrier(jnp.mean(normed_grad * normed, axis=-1, keepdims=True)))
        updates = (lax.optimization_barrier(jnp.sum(attend_grad * normed, axis=0)), lax.optimization_barrier(jnp.sum(attend_grad, axis=0)), lax.optimization_barrier(jnp.sum(feed_grad * normed, axis=0)), lax.optimization_barrier(jnp.sum(feed_grad, axis=0)), block_term(attend_in, projected_low), qkv_bias_part, block_term(context, row_cotangent), block_term(feed_in, hidden_low), up_bias_part, block_term(activated, row_cotangent), out_bias_part)
        carry = tuple((total + update for total, update in zip(carry, updates)))
        return (carry, (row_output, row_input_grad))
    start = (jnp.zeros((D,), jnp.float32), jnp.zeros((D,), jnp.float32), jnp.zeros((D,), jnp.float32), jnp.zeros((D,), jnp.float32), jnp.zeros((D, 3 * D), jnp.float32), jnp.zeros((3 * D,), jnp.float32), jnp.zeros((D, D), jnp.float32), jnp.zeros((D, FF), jnp.float32), jnp.zeros((FF,), jnp.float32), jnp.zeros((FF, D), jnp.float32), jnp.zeros((D,), jnp.float32))
    items = (layer_input.reshape(SEQS, SEQ_LEN, D), segment_ids, out_cotangent.reshape(SEQS, SEQ_LEN, D))
    totals, stacked = lax.scan(one_row, start, items)
    layer_output = stacked[0].reshape(TOKENS, D)
    input_grad = stacked[1].reshape(TOKENS, D)
    return (layer_output, input_grad, totals[0], totals[1], totals[2], totals[3], totals[4], totals[5], totals[6], totals[7], totals[8], totals[9], totals[10])
```

```python
import functools

import jax
import jax.numpy as jnp
from jax import lax
from jax.experimental import pallas as pl
from jax.experimental.pallas import tpu as pltpu
from jax.sharding import PartitionSpec as P

HEAD_DIM = 256
ROTARY = 64


EPS = 1e-05
SQRT_HALF = 0.7071067811865476
INV_ROOT_TAU = 0.3989422804014327
MASKED = -1e30
LANES = 128
VMEM_LIMIT = 56 * 1024 * 1024
LOW = jnp.bfloat16
WIDE = jnp.float32


def gelu_parts(pre):
    cdf = 0.5 * (1.0 + lax.erf(pre * SQRT_HALF))
    return (pre * cdf, cdf + pre * jnp.exp(-0.5 * pre * pre) * INV_ROOT_TAU)


def rotary_table(positions):
    half = ROTARY // 2
    freq = 10000.0 ** (-2.0 * jnp.arange(half).astype(WIDE) / ROTARY)
    lanes = jnp.concatenate([freq, freq, jnp.zeros((LANES - ROTARY,), WIDE)])
    angle = positions.astype(WIDE)[:, None] * lanes[None, :]
    return jnp.concatenate([jnp.cos(angle), jnp.sin(angle)], axis=1)


def turn(values, table, sign):
    half = ROTARY // 2
    first = values[:, :LANES]
    cosine, sine = table[:, :LANES], table[:, LANES:] * sign
    lane = lax.broadcasted_iota(jnp.int32, first.shape, 1)
    ahead = pltpu.roll(first, LANES - half, 1)
    behind = pltpu.roll(first, half, 1)
    first = first * cosine + jnp.where(lane < half, -ahead, behind) * sine
    return jnp.concatenate([first, values[:, LANES:]], axis=1)


def partners(size, bit):
    return [(i, i ^ bit) for i in range(size)]


def bits_of(size):
    if size & (size - 1):
        raise ValueError("axis size")
    return [1 << i for i in range(size.bit_length() - 1)]


def swap(value, axis, bit):
    return lax.ppermute(value, axis, partners(lax.axis_size(axis), bit))


def is_set(axis, bit):
    return (lax.axis_index(axis) & bit) != 0


def relative(value, axis):
    size = lax.axis_size(axis)
    for bit in bits_of(size):
        parts = jnp.split(value, size, axis=-1)
        turned = jnp.concatenate([parts[j ^ bit] for j in range(size)], axis=-1)
        value = jnp.where(is_set(axis, bit), turned, value)
    return value


def gather(shard, axis):
    pieces = {0: shard}
    for bit in reversed(bits_of(lax.axis_size(axis))):
        for j in sorted(pieces):
            pieces[j | bit] = swap(pieces[j], axis, bit)
    return [pieces[j] for j in range(len(pieces))]


def scatter_sum(pieces, axis):
    pieces = dict(enumerate(pieces))
    for bit in bits_of(lax.axis_size(axis)):
        for j in sorted(pieces):
            if j & bit:
                moved = swap(pieces.pop(j).astype(jnp.bfloat16), axis, bit)
                pieces[j ^ bit] = pieces[j ^ bit].astype(jnp.float32) + moved.astype(jnp.float32)
    return pieces[0]


def pair_sum(value, axis):
    for bit in bits_of(lax.axis_size(axis)):
        value = value.astype(jnp.bfloat16)
        moved = swap(value, axis, bit)
        value = value.astype(jnp.float32) + moved.astype(jnp.float32)
    return value


def wide_sum(value, axes):
    for axis in axes:
        for bit in bits_of(lax.axis_size(axis)):
            value = value + swap(value, axis, bit)
    return value


def line_sum(value, axis):
    size = lax.axis_size(axis)
    me = lax.axis_index(axis)
    if size == 4:
        moved = lax.ppermute(value, axis, [(0, 1), (3, 2)])
        value = (value.astype(WIDE) + moved.astype(WIDE)).astype(LOW)
        moved = lax.ppermute(value, axis, [(1, 2), (2, 1)])
        value = (value.astype(WIDE) + moved.astype(WIDE)).astype(LOW)
        sent = lax.ppermute(value, axis, [(1, 0), (2, 3)])
        return value, sent
    value = pair_sum(value, axis).astype(LOW)
    return value, value


def dot(a, b, dims):
    return lax.dot_general(a, b, (dims, ((), ())), preferred_element_type=WIDE)


def params(steps):
    return pltpu.CompilerParams(
        dimension_semantics=("arbitrary",) * steps, vmem_limit_bytes=VMEM_LIMIT
    )


def cost(flops, *arrays, exps=0):
    size = sum(a.size * a.dtype.itemsize for a in arrays)
    return pl.CostEstimate(flops=int(flops), bytes_accessed=int(size), transcendentals=int(exps))


def shape(dims, kind):
    return jax.ShapeDtypeStruct(dims, kind)


def whole(array):
    return pl.BlockSpec(array.shape, lambda *_: (0,) * len(array.shape))


def block_at(index, j, width):
    return pl.ds(pl.multiple_of((index ^ j) * width, width), width)


def norm_kernel(groups, me, x_ref, c_ref, v_ref, a_ref, f_ref, low_ref, stat_ref, sum_ref):
    width = x_ref.shape[1] // groups
    parts = [x_ref[:, block_at(me[0], j, width)].astype(WIDE) for j in range(groups)]
    total = x_ref.shape[1]
    mean = sum(jnp.sum(p, axis=1, keepdims=True) for p in parts) / total
    parts = [p - mean for p in parts]
    variance = sum(jnp.sum(p * p, axis=1, keepdims=True) for p in parts) / total
    scale = lax.rsqrt(variance + EPS)

    @pl.when(pl.program_id(0) == 0)
    def _():
        sum_ref[...] = jnp.zeros_like(sum_ref)

    for j in range(groups):
        here = block_at(me[0], j, width)
        there = slice(j * width, (j + 1) * width)
        normed = parts[j] * scale
        a_ref[:, there] = (normed * v_ref[0:1, here] + v_ref[1:2, here]).astype(LOW)
        f_ref[:, there] = (normed * v_ref[2:3, here] + v_ref[3:4, here]).astype(LOW)
        piece = c_ref[:, here]
        low_ref[:, there] = piece
        sum_ref[:, here] += jnp.sum(piece.astype(WIDE), axis=0, keepdims=True)
    stat_ref[:, :LANES] = jnp.broadcast_to(mean, (mean.shape[0], LANES))
    stat_ref[:, LANES:] = jnp.broadcast_to(scale, (mean.shape[0], LANES))


def norm_call(me, x, c, vectors, groups):
    rows, d = x.shape
    tile = min(256, rows)
    row = pl.BlockSpec((tile, d), lambda i, me: (i, 0))
    return pl.pallas_call(
        functools.partial(norm_kernel, groups),
        out_shape=(
            shape((rows, d), LOW),
            shape((rows, d), LOW),
            shape((rows, d), LOW),
            shape((rows, 2 * LANES), WIDE),
            shape((1, d), WIDE),
        ),
        grid_spec=pltpu.PrefetchScalarGridSpec(
            num_scalar_prefetch=1,
            grid=(rows // tile,),
            in_specs=[row, row, whole(vectors)],
            out_specs=[
                row,
                row,
                row,
                pl.BlockSpec((tile, 2 * LANES), lambda i, me: (i, 0)),
                pl.BlockSpec((1, d), lambda i, me: (0, 0)),
            ],
        ),
        compiler_params=params(1),
        cost_estimate=cost(20 * x.size, x, x, x, x, c),
        name="norm",
    )(me, x, c, vectors)


def project_kernel(groups, a_ref, *refs):
    pieces, (bias_ref, table_ref, q_ref, kv_ref) = refs[:groups], refs[groups:]
    depth = a_ref.shape[1] // groups
    acc = bias_ref[...]
    for j in range(groups):
        acc = acc + jnp.dot(
            a_ref[:, j * depth : (j + 1) * depth], pieces[j][...], preferred_element_type=WIDE
        )
    table = table_ref[...]
    q_ref[...] = turn(acc[:, :HEAD_DIM], table, 1.0).astype(LOW)
    kv_ref[:, :HEAD_DIM] = turn(acc[:, HEAD_DIM : 2 * HEAD_DIM], table, 1.0).astype(LOW)
    kv_ref[:, HEAD_DIM:] = acc[:, 2 * HEAD_DIM :].astype(LOW)


def project_call(a, pieces, bias, table):
    rows, d = a.shape
    groups = len(pieces)
    columns = pieces[0].shape[1]
    heads = columns // (3 * HEAD_DIM)
    tile = min(512, rows)
    return pl.pallas_call(
        functools.partial(project_kernel, groups),
        out_shape=(
            shape((rows, heads * HEAD_DIM), LOW),
            shape((rows, heads * 2 * HEAD_DIM), LOW),
        ),
        grid=(heads, rows // tile),
        in_specs=[pl.BlockSpec((tile, d), lambda h, i: (i, 0))]
        + [pl.BlockSpec((d // groups, 3 * HEAD_DIM), lambda h, i: (0, h))] * groups
        + [
            pl.BlockSpec((1, 3 * HEAD_DIM), lambda h, i: (0, h)),
            pl.BlockSpec((tile, 2 * LANES), lambda h, i: (i, 0)),
        ],
        out_specs=[
            pl.BlockSpec((tile, HEAD_DIM), lambda h, i: (i, h)),
            pl.BlockSpec((tile, 2 * HEAD_DIM), lambda h, i: (i, h)),
        ],
        compiler_params=params(2),
        cost_estimate=cost(2 * rows * d * columns, a, *pieces),
        name="project",
    )(a, *pieces, bias, table)


def allowed(seg_q, seg_k, row_at, key_at):
    q = lax.broadcasted_iota(jnp.int32, (seg_q.shape[0], seg_k.shape[1]), 0) + row_at
    k = lax.broadcasted_iota(jnp.int32, (seg_q.shape[0], seg_k.shape[1]), 1) + key_at
    return (seg_q == seg_k) & (k <= q)


def attend_kernel(tile, scale, low_ref, q_ref, past_ref, own_ref, sq_ref, sk_ref, o_ref, lse_ref, m, l, acc):
    i = pl.program_id(1)
    rows = own_ref.shape[0]
    count = rows // tile
    first = low_ref[i]
    m[...] = jnp.full_like(m, MASKED)
    l[...] = jnp.zeros_like(l)
    acc[...] = jnp.zeros_like(acc)
    q = q_ref[...]
    seg_q = sq_ref[...]

    def visit(kv_ref, c, key_at):
        here = pl.ds(pl.multiple_of(c * tile, tile), tile)
        k = kv_ref[here, :HEAD_DIM]
        v = kv_ref[here, HEAD_DIM:]
        seg_k = sk_ref[:, pl.ds(pl.multiple_of(key_at, tile), tile)]
        s = dot(q, k, ((1,), (1,))) * scale
        s = jnp.where(allowed(seg_q, seg_k, i * tile + rows, key_at), s, MASKED)
        top = jnp.maximum(m[...], jnp.max(s, axis=1, keepdims=True))
        fade = jnp.exp(m[...] - top)
        p = jnp.exp(s - top)
        l[...] = l[...] * fade + jnp.sum(p, axis=1, keepdims=True)
        acc[...] = acc[...] * fade + jnp.dot(p.astype(LOW), v, preferred_element_type=WIDE)
        m[...] = top

    @pl.loop(jnp.minimum(first, count), count)
    def _(c):
        visit(past_ref, c, c * tile)

    @pl.loop(jnp.maximum(first - count, 0), i + 1)
    def _(c):
        visit(own_ref, c, rows + c * tile)

    o_ref[...] = (acc[...] / l[...]).astype(LOW)
    lse_ref[...] = jnp.broadcast_to(m[...] + jnp.log(l[...]), lse_ref.shape)


def attend_call(low, q, past, own, seg_q, seg_k, tile, scale):
    rows = q.shape[0]
    heads = q.shape[1] // HEAD_DIM
    keys = pl.BlockSpec((rows, 2 * HEAD_DIM), lambda h, i, low: (0, h))
    pairs = heads * rows * rows
    return pl.pallas_call(
        functools.partial(attend_kernel, tile, scale),
        out_shape=(shape(q.shape, LOW), shape((rows, heads * LANES), WIDE)),
        grid_spec=pltpu.PrefetchScalarGridSpec(
            num_scalar_prefetch=1,
            grid=(heads, rows // tile),
            in_specs=[
                pl.BlockSpec((tile, HEAD_DIM), lambda h, i, low: (i, h)),
                keys,
                keys,
                pl.BlockSpec((tile, 1), lambda h, i, low: (i, 0)),
                whole(seg_k),
            ],
            out_specs=[
                pl.BlockSpec((tile, HEAD_DIM), lambda h, i, low: (i, h)),
                pl.BlockSpec((tile, LANES), lambda h, i, low: (i, h)),
            ],
            scratch_shapes=[
                pltpu.VMEM((tile, 1), WIDE),
                pltpu.VMEM((tile, 1), WIDE),
                pltpu.VMEM((tile, HEAD_DIM), WIDE),
            ],
        ),
        compiler_params=params(2),
        cost_estimate=cost(6 * pairs * HEAD_DIM, q, past, own, q, exps=2 * pairs),
        name="attend",
    )(low, q, past, own, seg_q, seg_k)


def attend_back_kernel(
    tile, scale, low_ref, q_ref, past_ref, own_ref, sq_ref, sk_ref, o_ref, lse_ref, g_ref,
    dq_ref, down_ref, dpast_ref, past_acc,
):
    rows = own_ref.shape[0]
    count = rows // tile
    dq_ref[...] = jnp.zeros_like(dq_ref)
    down_ref[...] = jnp.zeros_like(down_ref)
    past_acc[...] = jnp.zeros_like(past_acc)

    @pl.loop(0, count)
    def _(i):
        mine = pl.ds(pl.multiple_of(i * tile, tile), tile)
        first = low_ref[i]
        q = q_ref[mine, :]
        g = g_ref[mine, :]
        seg_q = sq_ref[mine, :]
        lse = lse_ref[mine, 0:1]
        delta = jnp.sum(g.astype(WIDE) * o_ref[mine, :].astype(WIDE), axis=1, keepdims=True)

        def visit(kv_ref, grad_ref, c, key_at):
            here = pl.ds(pl.multiple_of(c * tile, tile), tile)
            k = kv_ref[here, :HEAD_DIM]
            v = kv_ref[here, HEAD_DIM:]
            seg_k = sk_ref[:, pl.ds(pl.multiple_of(key_at, tile), tile)]
            s = dot(q, k, ((1,), (1,))) * scale
            p = jnp.where(
                allowed(seg_q, seg_k, i * tile + rows, key_at), jnp.exp(s - lse), 0.0
            )
            dp = dot(g, v, ((1,), (1,)))
            ds = (p * (dp - delta)).astype(LOW)
            grad_ref[here, HEAD_DIM:] += dot(p.astype(LOW), g, ((0,), (0,)))
            grad_ref[here, :HEAD_DIM] += dot(ds, q, ((0,), (0,))) * scale
            dq_ref[mine, :] += jnp.dot(ds, k, preferred_element_type=WIDE) * scale

        @pl.loop(jnp.minimum(first, count), count)
        def _(c):
            visit(past_ref, past_acc, c, c * tile)

        @pl.loop(jnp.maximum(first - count, 0), i + 1)
        def _(c):
            visit(own_ref, down_ref, c, rows + c * tile)

    dpast_ref[...] = past_acc[...].astype(LOW)


def attend_back_call(low, q, past, own, seg_q, seg_k, o, lse, g, tile, scale):
    rows = q.shape[0]
    heads = q.shape[1] // HEAD_DIM
    one = pl.BlockSpec((rows, HEAD_DIM), lambda h, low: (0, h))
    two = pl.BlockSpec((rows, 2 * HEAD_DIM), lambda h, low: (0, h))
    pairs = heads * rows * rows
    return pl.pallas_call(
        functools.partial(attend_back_kernel, tile, scale),
        out_shape=(shape(q.shape, WIDE), shape(own.shape, WIDE), shape(own.shape, LOW)),
        grid_spec=pltpu.PrefetchScalarGridSpec(
            num_scalar_prefetch=1,
            grid=(heads,),
            in_specs=[
                one,
                two,
                two,
                whole(seg_q),
                whole(seg_k),
                one,
                pl.BlockSpec((rows, LANES), lambda h, low: (0, h)),
                one,
            ],
            out_specs=[one, two, two],
            scratch_shapes=[pltpu.VMEM((rows, 2 * HEAD_DIM), WIDE)],
        ),
        compiler_params=params(1),
        cost_estimate=cost(15 * pairs * HEAD_DIM, q, past, own, own, own, exps=2 * pairs),
        name="attend_back",
    )(low, q, past, own, seg_q, seg_k, o, lse, g)


def finish_kernel(dq_ref, dkv_ref, back_ref, table_ref, p_ref, bias_ref):
    table = table_ref[...]

    @pl.when(pl.program_id(0) == 0)
    def _():
        bias_ref[...] = jnp.zeros_like(bias_ref)

    for h in range(dq_ref.shape[1] // HEAD_DIM):
        at = 2 * h * HEAD_DIM
        key = slice(at, at + HEAD_DIM)
        value = slice(at + HEAD_DIM, at + 2 * HEAD_DIM)
        parts = (
            turn(dq_ref[:, h * HEAD_DIM : (h + 1) * HEAD_DIM], table, -1.0),
            turn(dkv_ref[:, key] + back_ref[:, key].astype(WIDE), table, -1.0),
            dkv_ref[:, value] + back_ref[:, value].astype(WIDE),
        )
        for n, part in enumerate(parts):
            to = slice((3 * h + n) * HEAD_DIM, (3 * h + n + 1) * HEAD_DIM)
            p_ref[:, to] = part.astype(LOW)
            bias_ref[:, to] += jnp.sum(part, axis=0, keepdims=True)


def finish_call(dq, dkv, back, table):
    rows = dq.shape[0]
    columns = 3 * dq.shape[1]
    tile = min(256, rows)

    def spec(width):
        return pl.BlockSpec((tile, width), lambda i: (i, 0))

    return pl.pallas_call(
        finish_kernel,
        out_shape=(shape((rows, columns), LOW), shape((1, columns), WIDE)),
        grid=(rows // tile,),
        in_specs=[spec(dq.shape[1]), spec(dkv.shape[1]), spec(dkv.shape[1]), spec(2 * LANES)],
        out_specs=[spec(columns), pl.BlockSpec((1, columns), lambda i: (0, 0))],
        compiler_params=params(1),
        cost_estimate=cost(10 * rows * columns, dq, dkv, dkv),
        name="finish",
    )(dq, dkv, back, table)


def up_kernel(groups, f_ref, *refs):
    pieces, (bias_ref, act_ref, slope_ref) = refs[:groups], refs[groups:]
    depth = f_ref.shape[1] // groups
    half = f_ref.shape[0] // 2
    for r in range(2):
        at = slice(r * half, (r + 1) * half)
        acc = bias_ref[...]
        for j in range(groups):
            acc = acc + jnp.dot(
                f_ref[at, j * depth : (j + 1) * depth], pieces[j][...], preferred_element_type=WIDE
            )
        activated, slope = gelu_parts(acc)
        act_ref[at, :] = activated.astype(LOW)
        slope_ref[at, :] = slope


def up_call(f, pieces, bias):
    rows, d = f.shape
    groups = len(pieces)
    hidden = pieces[0].shape[1]
    tile = min(512, hidden)
    out = pl.BlockSpec((rows, tile), lambda n: (0, n))
    return pl.pallas_call(
        functools.partial(up_kernel, groups),
        out_shape=(shape((rows, hidden), LOW), shape((rows, hidden), WIDE)),
        grid=(hidden // tile,),
        in_specs=[whole(f)]
        + [pl.BlockSpec((d // groups, tile), lambda n: (0, n))] * groups
        + [pl.BlockSpec((1, tile), lambda n: (0, n))],
        out_specs=[out, out],
        compiler_params=params(1),
        cost_estimate=cost(2 * rows * d * hidden, f, f, f, *pieces),
        name="up",
    )(f, *pieces, bias)


def hidden_kernel(groups, c_ref, *refs):
    pieces, (slope_ref, h_ref, bias_ref) = refs[:groups], refs[groups:]
    depth = c_ref.shape[1] // groups
    half = c_ref.shape[0] // 2
    sums = 0.0
    for r in range(2):
        at = slice(r * half, (r + 1) * half)
        acc = 0.0
        for j in range(groups):
            acc = acc + dot(
                c_ref[at, j * depth : (j + 1) * depth], pieces[j][...], ((1,), (1,))
            )
        grad = acc * slope_ref[at, :]
        h_ref[at, :] = grad.astype(LOW)
        sums = sums + jnp.sum(grad, axis=0, keepdims=True)
    bias_ref[...] = sums


def hidden_call(c, pieces, slope):
    rows, d = c.shape
    groups = len(pieces)
    hidden = pieces[0].shape[0]
    tile = min(512, hidden)
    out = pl.BlockSpec((rows, tile), lambda n: (0, n))
    return pl.pallas_call(
        functools.partial(hidden_kernel, groups),
        out_shape=(shape((rows, hidden), LOW), shape((1, hidden), WIDE)),
        grid=(hidden // tile,),
        in_specs=[whole(c)]
        + [pl.BlockSpec((tile, d // groups), lambda n: (n, 0))] * groups
        + [out],
        out_specs=[out, pl.BlockSpec((1, tile), lambda n: (0, n))],
        compiler_params=params(1),
        cost_estimate=cost(2 * rows * d * hidden, c, c, c, *pieces),
        name="hidden",
    )(c, *pieces, slope)


def inward_kernel(me, h_ref, p_ref, up_ref, qkv_ref, x_ref, stat_ref, v_ref, n_ref, sum_ref):
    feed = dot(h_ref[...], up_ref[...], ((1,), (1,)))
    attend = dot(p_ref[...], qkv_ref[...], ((1,), (1,)))
    n_ref[...] = (attend * v_ref[0:1, :] + feed * v_ref[2:3, :]).astype(LOW)
    normed = (x_ref[...].astype(WIDE) - stat_ref[:, 0:1]) * stat_ref[:, LANES : LANES + 1]

    @pl.when(pl.program_id(0) == 0)
    def _():
        sum_ref[...] = jnp.zeros_like(sum_ref)

    sum_ref[0:1, :] += jnp.sum(attend * normed, axis=0, keepdims=True)
    sum_ref[1:2, :] += jnp.sum(attend, axis=0, keepdims=True)
    sum_ref[2:3, :] += jnp.sum(feed * normed, axis=0, keepdims=True)
    sum_ref[3:4, :] += jnp.sum(feed, axis=0, keepdims=True)


def inward_call(me, j, h, p, up, qkv, x, stat, vectors):
    rows = h.shape[0]
    width = up.shape[0]
    tile = min(256, rows)
    return pl.pallas_call(
        inward_kernel,
        out_shape=(shape((rows, width), LOW), shape((8, width), WIDE)),
        grid_spec=pltpu.PrefetchScalarGridSpec(
            num_scalar_prefetch=1,
            grid=(rows // tile,),
            in_specs=[
                pl.BlockSpec((tile, h.shape[1]), lambda i, me: (i, 0)),
                pl.BlockSpec((tile, p.shape[1]), lambda i, me: (i, 0)),
                whole(up),
                whole(qkv),
                pl.BlockSpec((tile, width), lambda i, me: (i, me[0] ^ j)),
                pl.BlockSpec((tile, stat.shape[1]), lambda i, me: (i, 0)),
                pl.BlockSpec((vectors.shape[0], width), lambda i, me: (0, me[0] ^ j)),
            ],
            out_specs=[
                pl.BlockSpec((tile, width), lambda i, me: (i, 0)),
                pl.BlockSpec((8, width), lambda i, me: (0, 0)),
            ],
        ),
        compiler_params=params(1),
        cost_estimate=cost(2 * rows * width * (h.shape[1] + p.shape[1]), h, p, up, qkv),
        name="inward",
    )(me, h, p, up, qkv, x, stat, vectors)


def chosen(flags, held, sent):
    return jnp.where(flags[1] > 0, held[...], sent[...]).astype(WIDE)


def output_kernel(groups, flags, x_ref, v_ref, *refs):
    held, sent, out_ref = refs[:groups], refs[groups : 2 * groups], refs[2 * groups]
    width = x_ref.shape[1] // groups
    for j in range(groups):
        here = block_at(flags[0], j, width)
        total = x_ref[:, here].astype(WIDE) + chosen(flags, held[j], sent[j]) + v_ref[4:5, here]
        out_ref[:, here] = total.astype(LOW)


def input_grad_kernel(groups, flags, x_ref, c_ref, stat_ref, *refs):
    held, sent, out_ref = refs[:groups], refs[groups : 2 * groups], refs[2 * groups]
    total = x_ref.shape[1]
    width = total // groups
    mean, scale = stat_ref[:, 0:1], stat_ref[:, LANES : LANES + 1]
    plain, mixed = 0.0, 0.0
    for j in range(groups):
        grad = chosen(flags, held[j], sent[j])
        normed = (x_ref[:, block_at(flags[0], j, width)].astype(WIDE) - mean) * scale
        plain = plain + jnp.sum(grad, axis=1, keepdims=True)
        mixed = mixed + jnp.sum(grad * normed, axis=1, keepdims=True)
    plain, mixed = plain / total, mixed / total
    for j in range(groups):
        here = block_at(flags[0], j, width)
        grad = chosen(flags, held[j], sent[j])
        normed = (x_ref[:, here].astype(WIDE) - mean) * scale
        out_ref[:, here] = c_ref[:, here].astype(WIDE) + scale * (grad - plain - normed * mixed)


def token_call(kernel, flags, arrays, chunks, kind, name):
    held, sent = [c[0] for c in chunks], [c[1] for c in chunks]
    groups = len(held)
    rows, d = arrays[0].shape
    tile = min(256, rows)

    def spec(a):
        if a.shape[0] == rows:
            return pl.BlockSpec((tile, a.shape[1]), lambda i, flags: (i, 0))
        return whole(a)

    inputs = list(arrays) + held + sent
    return pl.pallas_call(
        functools.partial(kernel, groups),
        out_shape=shape((rows, d), kind),
        grid_spec=pltpu.PrefetchScalarGridSpec(
            num_scalar_prefetch=1,
            grid=(rows // tile,),
            in_specs=[spec(a) for a in inputs],
            out_specs=pl.BlockSpec((tile, d), lambda i, flags: (i, 0)),
        ),
        compiler_params=params(1),
        cost_estimate=cost(10 * rows * d, *inputs),
        name=name,
    )(flags, *inputs)


def after(value, *others):
    return lax.optimization_barrier((value, *others))[0]


def shards(
    layer_input,
    attention_gain,
    attention_shift,
    feed_gain,
    feed_shift,
    qkv_weight,
    qkv_bias,
    dense_weight,
    up_weight,
    up_bias,
    down_weight,
    out_bias,
    segment_ids,
    out_cotangent,
):
    rows, d = layer_input.shape
    scale = HEAD_DIM ** (-0.5)
    groups = lax.axis_size("dp")
    lines = lax.axis_size("tensor")
    if lax.axis_size("ctx") != 2:
        raise ValueError("ctx size")
    later = lax.axis_index("ctx") > 0
    forward, backward = [(0, 1)], [(1, 0)]
    line_at = lax.axis_index("tensor")
    me = lax.axis_index("dp").reshape(1)
    inner = (line_at > 0) & (line_at < lines - 1)
    flags = jnp.stack([lax.axis_index("dp"), inner.astype(jnp.int32)])
    far = groups // 2

    qkv = gather(qkv_weight, "dp")
    up = gather(after(up_weight, qkv[far]), "dp")
    dense = gather(after(dense_weight, up[far]), "dp")
    down = gather(after(down_weight, dense[far]), "dp")

    own_segments = segment_ids[0]
    past_segments = lax.ppermute(own_segments, "ctx", forward)
    tile = min(512, rows)
    count = rows // tile
    key_segments = jnp.concatenate([past_segments, own_segments])
    lowest = own_segments[::tile]
    highest = key_segments[tile - 1 :: tile]
    unreached = (highest[None, :] < lowest[:, None]) | (
        (jnp.arange(2 * count)[None, :] < count) & ~later
    )
    skipped = jnp.sum(unreached.astype(jnp.int32), axis=1)
    seg_q = own_segments[:, None]
    seg_k = key_segments[None, :]
    positions = lax.axis_index("ctx") * rows + jnp.arange(rows, dtype=jnp.int32)
    table = rotary_table(positions)
    zero = jnp.zeros_like(out_bias)
    vectors = jnp.stack(
        [attention_gain, attention_shift, feed_gain, feed_shift, out_bias, zero, zero, zero]
    )

    attend_in, feed_in, cotangent_low, stat, cotangent_part = norm_call(
        me, layer_input, out_cotangent, vectors, groups
    )
    queries, own = project_call(attend_in, qkv, qkv_bias[None], table)
    past = lax.ppermute(own, "ctx", forward)
    activated, slope = up_call(feed_in, up, up_bias[None])
    context, lse = attend_call(skipped, queries, past, own, seg_q, seg_k, tile, scale)

    full_dense = jnp.concatenate(dense, axis=1)
    context_grad = dot(cotangent_low, full_dense, ((1,), (1,))).astype(LOW)
    dq, dkv, dpast = attend_back_call(
        skipped, queries, past, own, seg_q, seg_k, context, lse, context_grad, tile, scale
    )
    back = lax.ppermute(dpast, "ctx", backward)

    outs = []
    for j in range(groups):
        part = dot(context, dense[j], ((1,), (0,))) + dot(activated, down[j], ((1,), (0,)))
        outs.append(line_sum(part.astype(LOW), "tensor"))
    layer_output = token_call(
        output_kernel, flags, (layer_input, vectors), outs, LOW, "layer_output"
    )

    hidden_low, up_bias_part = hidden_call(cotangent_low, down, slope)
    projected_low, qkv_bias_part = finish_call(dq, dkv, back, table)
    grads, gain_parts = [], []
    for j in range(groups):
        part, sums = inward_call(
            me, j, hidden_low, projected_low, up[j], qkv[j], layer_input, stat, vectors
        )
        grads.append(line_sum(part, "tensor"))
        gain_parts.append(sums[:4])
    input_grad = token_call(
        input_grad_kernel, flags, (layer_input, out_cotangent, stat), grads, WIDE, "input_grad"
    )

    def row_pieces(left, right):
        return [dot(part, right, ((0,), (0,))) for part in jnp.split(left, groups, axis=1)]

    def column_pieces(left, right):
        return [dot(left, part, ((0,), (0,))) for part in jnp.split(right, groups, axis=1)]

    def weight_grad(pieces):
        low = [piece.astype(LOW) for piece in pieces]
        return pair_sum(scatter_sum(low, "dp"), "ctx")

    dense_weight_grad = weight_grad(column_pieces(context, cotangent_low))
    down_weight_grad = weight_grad(column_pieces(activated, cotangent_low))
    up_weight_grad = weight_grad(row_pieces(feed_in, hidden_low))
    qkv_weight_grad = weight_grad(row_pieces(attend_in, projected_low))

    gains = relative(jnp.concatenate(gain_parts, axis=1), "dp").reshape(-1)
    gain_sums = wide_sum(gains, ("tensor",))
    small = jnp.concatenate([gain_sums, cotangent_part[0], qkv_bias_part[0], up_bias_part[0]])
    small = wide_sum(small, ("dp", "ctx"))
    edges = [d, 2 * d, 3 * d, 4 * d, 5 * d, 5 * d + qkv_bias.shape[0]]
    (
        attention_gain_grad,
        attention_shift_grad,
        feed_gain_grad,
        feed_shift_grad,
        out_bias_grad,
        qkv_bias_grad,
        up_bias_grad,
    ) = jnp.split(small, edges)
    return (
        layer_output,
        input_grad,
        attention_gain_grad,
        attention_shift_grad,
        feed_gain_grad,
        feed_shift_grad,
        qkv_weight_grad,
        qkv_bias_grad,
        dense_weight_grad,
        up_weight_grad,
        up_bias_grad,
        down_weight_grad,
        out_bias_grad,
    )


def solution(mesh):
    in_specs = (
        P(("dp", "ctx"), None),
        P(),
        P(),
        P(),
        P(),
        P("dp", "tensor"),
        P("tensor"),
        P("tensor", "dp"),
        P("dp", "tensor"),
        P("tensor"),
        P("tensor", "dp"),
        P(),
        P("dp", "ctx"),
        P(("dp", "ctx"), None),
    )
    out_specs = (
        P(("dp", "ctx"), None),
        P(("dp", "ctx"), None),
        P(),
        P(),
        P(),
        P(),
        P("dp", "tensor"),
        P("tensor"),
        P("tensor", "dp"),
        P("dp", "tensor"),
        P("tensor"),
        P("tensor", "dp"),
        P(),
    )
    return jax.shard_map(shards, mesh=mesh, in_specs=in_specs, out_specs=out_specs, check_vma=False)
```
